256 devices in a mesh: section: 4 (over x_hi, core), dp: 64 (over y, x_lo, z).
Axes of the slice: x: 4 (x_hi: 2, x_lo: 2; x = x_hi * 2 + x_lo), y: 4, z: 8, core: 2. Of those that a mesh axis runs over, the one named last changes fastest.
Arguments:
- activations: bfloat16 [12288, 8, 4096], P('dp', 'section'), may hold values from -8 to 8
- damping: float32 [8], P('section'), may hold values from 0.1 to 1
Outputs:
- schur_inverse: float32 [256, 128, 128], P(('section', 'dp'))
- coupling: float32 [256, 128, 128], P(('section', 'dp'))
The draws below stay inside these ranges and needn't reach their ends.
All inputs are finite; a program needn't handle non-finite values.
Results may differ from the reference program's by a relative error of at most 0.0003.
Values may be sent and summed in bfloat16 or wider, within the bound.
No kernel may reach another device: no remote copies, remote signals or barrier semaphores. Data moves between devices by JAX's collectives and lax.ppermute only.
A program may use at most 64 MiB of HBM per device.

```python
import math
from functools import partial
import jax
import jax.numpy as jnp
from jax import lax

D = 4096
B = 128
TOK_DEV = 192
L = 8
NB = 32
TOKENS = 12288


def column_filter():
    rows_idx = jnp.arange(B)[:, None]
    cols_idx = jnp.arange(B)[None, :]
    lag_power = jnp.maximum(rows_idx - cols_idx, 0).astype(jnp.float32)
    fresh_weight = jnp.where(cols_idx == 0, 1.0, jnp.sqrt(1.0 - 0.9 * 0.9)).astype(jnp.float32)
    weights = jnp.power(jnp.float32(0.9), lag_power) * fresh_weight
    return jnp.where(rows_idx >= cols_idx, weights, 0.0).astype(jnp.float32)


def draw_activations(key, part):
    shared_key = jax.random.fold_in(key, 11)
    fresh_key = jax.random.fold_in(key, 23)
    shard_key = jax.random.fold_in(key, 41)
    column_key = jax.random.fold_in(key, 53)
    shared_part = jax.random.normal(shared_key, (TOKENS, 1, D), jnp.float32)
    fresh_part = jax.random.normal(fresh_key, (TOKENS, L, D), jnp.float32)
    token_scale = jnp.ones((TOKENS, 1, 1), jnp.float32)
    shard_scale = jnp.exp(jax.random.uniform(shard_key, (TOKENS // TOK_DEV, 1, 1, 1), jnp.float32, -0.7, 0.7))
    column_scale = jnp.exp(jax.random.uniform(column_key, (1, L, D), jnp.float32, -0.7, 0.7))
    mixture = 0.75 * shared_part + 0.66 * fresh_part
    mixture = mixture.reshape(TOKENS, L, NB, B)
    mixture = jnp.einsum('tlgi,ji->tlgj', mixture, column_filter(), precision=lax.Precision.HIGHEST)
    mixture = mixture.reshape(TOKENS, L, D) * token_scale * column_scale
    mixture = (mixture.reshape(TOKENS // TOK_DEV, TOK_DEV, L, D) * shard_scale).reshape(TOKENS, L, D)
    return jnp.clip(mixture, -8.0, 8.0).astype(jnp.bfloat16)


def block_levels(key, shape, cuts, least, high):
    gain, own = 1.0, jax.random.fold_in(key, 6)
    for position, shards_of in cuts:
        heights = jnp.exp(jax.random.uniform(jax.random.fold_in(own, position), (shards_of,), jnp.float32, least / len(cuts), high / len(cuts)))
        gain = gain * jnp.repeat(heights, shape[position] // shards_of).reshape([-1 if axis == position else 1 for axis in range(len(shape))])
    return gain


def setup_inputs(seed: int = 0) -> dict:
    key_of = jax.random.split(jax.random.key(seed), 3)
    activations = draw_activations(jax.random.fold_in(key_of[2], 71), 0)
    damping = jnp.clip(jnp.exp(math.log(1.0) - 2.3025851 * jax.random.uniform(key_of[1], (L,), jnp.float32) ** block_levels(key_of[1], (L,), ((0, 4),), -0.2, 0.2)), 0.1, 1.0)
    return dict(activations=activations, damping=damping)


def layer_grams(activations, index):
    current = lax.dynamic_index_in_dim(activations, index, 1, keepdims=False)
    current = current.astype(jnp.float32).reshape(TOKENS, NB, B)
    later = jnp.minimum(index + 1, L - 1).astype(jnp.int32)
    following = lax.dynamic_index_in_dim(activations, later, 1, keepdims=False)
    following = following.astype(jnp.float32).reshape(TOKENS, NB, B)
    diagonal = jnp.einsum('tgb,tgc->gbc', current, current, precision=lax.Precision.HIGHEST) / TOKENS
    crossed = jnp.einsum('tgb,tgc->gbc', current, following, precision=lax.Precision.HIGHEST) / TOKENS
    return (diagonal, crossed)

def solve_block(system, right_side):
    factor = jnp.linalg.cholesky(system)
    return jax.scipy.linalg.cho_solve((factor, True), right_side)

def reference(activations, damping):
    diagonal_gram, cross_gram = lax.map(partial(layer_grams, activations), jnp.arange(L, dtype=jnp.int32))
    trace_mean = jnp.sum(jnp.trace(diagonal_gram, axis1=2, axis2=3), axis=1) / D
    identity = jnp.eye(B, dtype=jnp.float32)
    damped = diagonal_gram + (damping * trace_mean)[:, None, None, None] * identity
    final_mask = (jnp.arange(L) == L - 1)[:, None, None, None]
    following = jnp.concatenate([damped[1:], damped[:1]], axis=0)
    following = jnp.where(final_mask, identity, following)
    cross_gram = jnp.where(final_mask, jnp.zeros_like(cross_gram), cross_gram)
    damped = damped.reshape(L * NB, B, B)
    following = following.reshape(L * NB, B, B)
    cross_gram = cross_gram.reshape(L * NB, B, B)
    coupling_t = jax.vmap(solve_block)(following, jnp.swapaxes(cross_gram, 1, 2))
    schur = damped - jnp.matmul(cross_gram, coupling_t, precision=lax.Precision.HIGHEST)
    identities = jnp.broadcast_to(identity, schur.shape)
    schur_inverse = jax.vmap(solve_block)(schur, identities)
    return (schur_inverse, jnp.swapaxes(coupling_t, 1, 2))
```

```python
from functools import partial

import jax
import jax.numpy as jnp
from jax import lax
from jax.experimental import pallas as pl
from jax.experimental.pallas import tpu as pltpu
from jax.sharding import PartitionSpec as P

B = 128
EVERY = ("section", "dp")


def dp_index(y1, y0, xl, z2, z1, z0):
    return ((((y1 * 2 + y0) * 2 + xl) * 2 + z2) * 2 + z1) * 2 + z0


def flipped(section):
    return section // 2


BITS = [tuple((d >> s) & 1 for s in (5, 4, 3, 2, 1, 0)) for d in range(64)]


def column_groups():
    groups = []
    for section in range(4):
        for z2 in range(2):
            for z1 in range(2):
                groups.append(
                    [
                        section * 64 + dp_index(m >> 3, (m >> 2) & 1, ((m >> 1) & 1) ^ flipped(section), z2, z1, m & 1)
                        for m in range(16)
                    ]
                )
    return groups


def following_route():
    route = []
    for section in range(1, 4):
        turn = flipped(section) ^ flipped(section - 1)
        for d, (y1, y0, xl, z2, z1, z0) in enumerate(BITS):
            route.append((section * 64 + d, (section - 1) * 64 + dp_index(y1, y0, xl ^ turn, z2, z1, z0)))
    return route


def home_route(a, b):
    route = []
    for section in range(4):
        turn = flipped(section)
        for d, (y1, y0, xl, z2, z1, z0) in enumerate(BITS):
            route.append((section * 64 + d, section * 64 + dp_index(z1 ^ a, y0, xl ^ turn, z2 ^ b, y1, z0)))
    return route


def gram_kernel(pos_ref, x0_ref, x1_ref, x2_ref, *out_refs):
    turn, z2, z1 = pos_ref[0], pos_ref[1], pos_ref[2]
    chunks, rows, _ = x0_ref.shape
    row = lax.broadcasted_iota(jnp.int32, (B, B), 0)
    col = lax.broadcasted_iota(jnp.int32, (B, B), 1)
    dims = (((0,), (0,)), ((), ()))
    half = chunks // 2

    def gram(left, right):
        return lax.dot_general(left, right, dims, preferred_element_type=jnp.float32)

    for zz in range(2):
        cols = pl.ds(zz * B, B)
        totals = [jnp.zeros((B, B), jnp.float32) for _ in range(5)]
        for j in range(chunks):
            x0 = x0_ref[j, :, cols]
            x1 = x1_ref[j, :, cols]
            x2 = x2_ref[j ^ (turn * 2), :, cols]
            for i, (p, q) in enumerate(((x0, x0), (x1, x1), (x2, x2), (x0, x1), (x1, x2))):
                totals[i] = totals[i] + gram(p, q)
        d0, d1, d2, c01, c12 = totals
        for layer, (d, n, c) in enumerate(((d0, d1, c01), (d1, d2, c12))):
            packed = jnp.where(row >= col, d, n)
            edge = jnp.sum(jnp.where(row == col, n, 0.0), axis=0, keepdims=True)
            edge = jnp.broadcast_to(edge, (8, B))
            for b in range(2):
                for a in range(2):

                    @pl.when(jnp.logical_and((z2 ^ b) == zz, (z1 ^ a) == layer))
                    def _():
                        out = out_refs[a * 2 + b]
                        out[0:B, :] = c
                        out[B : 2 * B, :] = packed
                        out[2 * B : 2 * B + 8, :] = edge


def partial_grams(x0, x1, x2, position):
    vmem = pl.BlockSpec(memory_space=pltpu.VMEM)
    return pl.pallas_call(
        gram_kernel,
        out_shape=[jax.ShapeDtypeStruct((2 * B + 8, B), jnp.float32)] * 4,
        in_specs=[pl.BlockSpec(memory_space=pltpu.SMEM), vmem, vmem, vmem],
        out_specs=[vmem] * 4,
        name="partial_grams",
        cost_estimate=pl.CostEstimate(flops=10 * 3072 * B * B * 2, bytes_accessed=6 * 3072 * B * 2, transcendentals=0),
        compiler_params=pltpu.CompilerParams(vmem_limit_bytes=24 * 2**20),
    )(position, x0, x1, x2)


def solve_block(system, right_side):
    factor = jnp.linalg.cholesky(system)
    return jax.scipy.linalg.cho_solve((factor, True), right_side)


def local(activations, damping):
    token_rows, local_layers, model_width = activations.shape
    group_size = lax.axis_size("dp")
    section_count = lax.axis_size("section")
    tokens_all = token_rows * group_size
    section = lax.axis_index("section")
    dp = lax.axis_index("dp")
    owner_layer = dp // 32
    z2, z1 = (dp >> 2) & 1, (dp >> 1) & 1
    groups = column_groups()

    def by_member(layer):
        cut = activations[:, layer, :].reshape(token_rows, 2, 2, 2, 2, 2, B)
        return cut.transpose(4, 1, 2, 5, 0, 3, 6).reshape(16, token_rows, 2 * B)

    def exchanged(columns):
        return lax.all_to_all(columns, EVERY, split_axis=0, concat_axis=0, axis_index_groups=groups, tiled=True)

    x0 = exchanged(by_member(0))
    squares = jnp.sum(jnp.square(activations.astype(jnp.float32)), axis=(0, 2))
    copies = jnp.broadcast_to(squares, (group_size, 1, local_layers))
    squares = lax.all_to_all(copies, "dp", split_axis=0, concat_axis=0, tiled=True)
    levels = damping * (jnp.sum(squares, axis=(0, 1)) / tokens_all) / model_width
    next_level = lax.ppermute(levels, "section", [(i, i - 1) for i in range(1, section_count)])
    x2 = lax.ppermute(x0, EVERY, following_route())
    x1 = exchanged(by_member(1))
    position = jnp.stack([(section == 1).astype(jnp.int32), z2.astype(jnp.int32), z1.astype(jnp.int32)])
    sent = partial_grams(x0, x1, x2, position)
    arrived = [lax.ppermute(sent[a * 2 + b], EVERY, home_route(a, b)) for a in range(2) for b in range(2)]
    owned = sum(arrived[1:], arrived[0]) / tokens_all

    identity = jnp.eye(B, dtype=jnp.float32)
    cross_gram, packed, edge = owned[:B], owned[B : 2 * B], owned[2 * B]
    lower = jnp.tril(packed, -1)
    upper = jnp.triu(packed, 1)
    level = jnp.where(owner_layer == 0, levels[0], levels[1])
    level_after = jnp.where(owner_layer == 0, levels[1], next_level[0])
    damped = lower + lower.T + packed * identity + level * identity
    following = upper + upper.T + edge[:, None] * identity + level_after * identity
    final_layer = jnp.logical_and(section == section_count - 1, owner_layer == local_layers - 1)
    system = jnp.where(final_layer, identity, following)
    cross_gram = jnp.where(final_layer, jnp.zeros_like(cross_gram), cross_gram)
    coupling_t = solve_block(system, cross_gram.T)
    schur = damped - jnp.matmul(cross_gram, coupling_t, precision=lax.Precision.HIGHEST)
    schur_inverse = solve_block(schur, identity)
    return (schur_inverse[None], coupling_t.T[None])


def solution(mesh):
    placed = (P("dp", "section", None), P("section"))
    return jax.shard_map(
        local,
        mesh=mesh,
        in_specs=placed,
        out_specs=(P(("section", "dp"), None, None), P(("section", "dp"), None, None)),
        check_vma=False,
    )
```

```python
from functools import partial

import jax
import jax.numpy as jnp
from jax import lax
from jax.experimental import pallas as pl
from jax.experimental.pallas import tpu as pltpu
from jax.sharding import PartitionSpec as P

B = 128
PANEL = 8
PARTS = 3
EVERY = ("section", "dp")


def dp_index(y1, y0, xl, z2, z1, z0):
    return ((((y1 * 2 + y0) * 2 + xl) * 2 + z2) * 2 + z1) * 2 + z0


def flipped(section):
    return section // 2


BITS = [tuple((d >> s) & 1 for s in (5, 4, 3, 2, 1, 0)) for d in range(64)]


def column_groups():
    groups = []
    for section in range(4):
        for z2 in range(2):
            for z1 in range(2):
                groups.append(
                    [
                        section * 64 + dp_index(m >> 3, (m >> 2) & 1, ((m >> 1) & 1) ^ flipped(section), z2, z1, m & 1)
                        for m in range(16)
                    ]
                )
    return groups


def following_route():
    route = []
    for section in range(1, 4):
        turn = flipped(section) ^ flipped(section - 1)
        for d, (y1, y0, xl, z2, z1, z0) in enumerate(BITS):
            route.append((section * 64 + d, (section - 1) * 64 + dp_index(y1, y0, xl ^ turn, z2, z1, z0)))
    return route


def home_route(a, b):
    route = []
    for section in range(4):
        turn = flipped(section)
        for d, (y1, y0, xl, z2, z1, z0) in enumerate(BITS):
            route.append((section * 64 + d, section * 64 + dp_index(z1 ^ a, y0, xl ^ turn, z2 ^ b, y1, z0)))
    return route


def member_block(m, zz):
    z1, y0, xl, z0 = m >> 3, (m >> 2) & 1, (m >> 1) & 1, m & 1
    return (((y0 * 2 + xl) * 2 + zz) * 2 + z1) * 2 + z0


def parts_of(value):
    parts = []
    for _ in range(PARTS):
        part = value.astype(jnp.bfloat16)
        parts.append(part)
        value = value - part.astype(jnp.float32)
    return parts


def columns_kernel(layer, damping_ref, x_ref, out_ref):
    groups = x_ref.shape[0]
    squares = jnp.zeros((PANEL, B), jnp.float32)
    for m in range(16):
        for zz in range(2):
            k = member_block(m, zz)
            cut = x_ref[:, layer, :, k * B : (k + 1) * B]
            out_ref[m, zz * groups : (zz + 1) * groups] = cut
            wide = cut.astype(jnp.float32)
            squares = squares + jnp.sum(wide * wide, axis=0)
    squares = jnp.broadcast_to(jnp.sum(squares, axis=0, keepdims=True), (PANEL, B))
    damping = jnp.full((PANEL, B), damping_ref[layer])
    row = lax.broadcasted_iota(jnp.int32, (PANEL, B), 0)
    extra = jnp.zeros((PANEL, B), jnp.float32)
    for i, part in enumerate(parts_of(squares) + parts_of(damping)):
        extra = jnp.where(row == i, part.astype(jnp.float32), extra)
    extra = extra.astype(jnp.bfloat16)
    for m in range(16):
        out_ref[m, 2 * groups] = extra


def sent_columns(x, damping, layer):
    groups = x.shape[0]
    vmem = pl.BlockSpec(memory_space=pltpu.VMEM)
    out = pl.pallas_call(
        partial(columns_kernel, layer),
        out_shape=jax.ShapeDtypeStruct((16, 2 * groups + 1, PANEL, B), jnp.bfloat16),
        in_specs=[pl.BlockSpec(memory_space=pltpu.SMEM), vmem],
        out_specs=vmem,
        name="sent_columns",
        cost_estimate=pl.CostEstimate(flops=2 * 2**20, bytes_accessed=2 * 2**21, transcendentals=0),
        compiler_params=pltpu.CompilerParams(vmem_limit_bytes=16 * 2**20),
    )(damping, x)
    return out.reshape(16, (2 * groups + 1) * PANEL, B)


def level_rows(x_ref):
    rows = x_ref.shape[1]
    total = jnp.zeros((PANEL, B), jnp.float32)
    for j in range(x_ref.shape[0]):
        total = total + x_ref[j, rows - PANEL :, :].astype(jnp.float32)
    last = x_ref[0, rows - PANEL :, :].astype(jnp.float32)
    squares = jnp.sum(total[:PARTS], axis=0, keepdims=True)
    damping = jnp.sum(last[PARTS : 2 * PARTS], axis=0, keepdims=True)
    return squares, damping * 0.25


def gram_kernel(pos_ref, x0_ref, x1_ref, x2_ref, *out_refs):
    turn, z2, z1 = pos_ref[0], pos_ref[1], pos_ref[2]
    chunks = x0_ref.shape[0]
    rows = (x0_ref.shape[1] - PANEL) // 2
    row = lax.broadcasted_iota(jnp.int32, (B, B), 0)
    col = lax.broadcasted_iota(jnp.int32, (B, B), 1)
    dims = (((0,), (0,)), ((), ()))

    def gram(left, *rights):
        right = jnp.concatenate(rights, axis=1) if len(rights) > 1 else rights[0]
        return lax.dot_general(left, right, dims, preferred_element_type=jnp.float32)

    levels = [level_rows(x_ref) for x_ref in (x0_ref, x1_ref, x2_ref)]
    for zz in range(2):
        cut = pl.ds(zz * rows, rows)
        first = jnp.zeros((B, 2 * B), jnp.float32)
        second = jnp.zeros((B, 2 * B), jnp.float32)
        third = jnp.zeros((B, B), jnp.float32)
        for j in range(chunks):
            x0 = x0_ref[j, cut, :]
            x1 = x1_ref[j, cut, :]
            x2 = x2_ref[j ^ (turn * 2), cut, :]
            first = first + gram(x0, x0, x1)
            second = second + gram(x1, x1, x2)
            third = third + gram(x2, x2)
        d0, d1, d2, c01, c12 = first[:, :B], second[:, :B], third, first[:, B:], second[:, B:]
        for layer, (d, n, c) in enumerate(((d0, d1, c01), (d1, d2, c12))):
            packed = jnp.where(row >= col, d, n)
            edge = jnp.sum(jnp.where(row == col, n, 0.0), axis=0, keepdims=True)
            for b in range(2):
                for a in range(2):

                    @pl.when(jnp.logical_and((z2 ^ b) == zz, (z1 ^ a) == layer))
                    def _():
                        out = out_refs[a * 2 + b]
                        out[0:B, :] = c
                        out[B : 2 * B, :] = packed
                        out[2 * B : 2 * B + 1, :] = edge
                        for i in range(2):
                            out[2 * B + 1 + i : 2 * B + 2 + i, :] = levels[layer + i][0]
                            out[2 * B + 3 + i : 2 * B + 4 + i, :] = levels[layer + i][1]
                        out[2 * B + 5 : 2 * B + 8, :] = jnp.zeros((3, B), jnp.float32)


def partial_grams(x0, x1, x2, position):
    vmem = pl.BlockSpec(memory_space=pltpu.VMEM)
    return pl.pallas_call(
        gram_kernel,
        out_shape=[jax.ShapeDtypeStruct((2 * B + PANEL, B), jnp.float32)] * 4,
        in_specs=[pl.BlockSpec(memory_space=pltpu.SMEM), vmem, vmem, vmem],
        out_specs=[vmem] * 4,
        name="partial_grams",
        cost_estimate=pl.CostEstimate(flops=10 * 3072 * B * B * 2, bytes_accessed=6 * 3072 * B * 2, transcendentals=0),
        compiler_params=pltpu.CompilerParams(vmem_limit_bytes=24 * 2**20),
    )(position, x0, x1, x2)


def inverted(panels):
    sub = lax.broadcasted_iota(jnp.int32, (PANEL, B), 0)
    lane = lax.broadcasted_iota(jnp.int32, (PANEL, B), 1)
    count = B // PANEL
    panels = list(panels)
    for k in range(count):
        first = k * PANEL
        here = jnp.logical_and(lane >= first, lane < first + PANEL)
        spread = [[jnp.broadcast_to(p[:, first + j : first + j + 1], (PANEL, B)) for j in range(PANEL)] for p in panels]
        own = spread[k]
        panel = jnp.where(here, jnp.where(lane - first == sub, 1.0, 0.0), panels[k])
        for j in range(PANEL):
            scale = 1.0 / own[j][j : j + 1, :]
            for q in range(j + 1, PANEL):
                top = own[q][j : j + 1, :] * scale
                own[q] = jnp.where(sub == j, top, own[q] - own[j] * top)
            top = panel[j : j + 1, :] * scale
            panel = jnp.where(sub == j, top, panel - own[j] * top)
        tops = [jnp.broadcast_to(panel[j : j + 1, :], (PANEL, B)) for j in range(PANEL)]
        for i in range(count):
            if i != k:
                rest = jnp.where(here, 0.0, panels[i])
                for j in range(PANEL):
                    rest = rest - spread[i][j] * tops[j]
                panels[i] = rest
        panels[k] = panel
    return panels


def cut_panels(square):
    return [square[i * PANEL : (i + 1) * PANEL, :] for i in range(B // PANEL)]


def solve_kernel(tokens, width, last_ref, *refs):
    arrived, (inverse_ref, coupling_ref) = refs[:4], refs[4:]
    owned = arrived[0][...] + arrived[1][...] + arrived[2][...] + arrived[3][...]
    row = lax.broadcasted_iota(jnp.int32, (B, B), 0)
    col = lax.broadcasted_iota(jnp.int32, (B, B), 1)
    edge = owned[2 * B :]
    mean = jnp.sum(edge, axis=1, keepdims=True) / tokens / width
    level, level_after = mean[1:2] * edge[3:4], mean[2:3] * edge[4:5]
    packed = owned[B : 2 * B] / tokens
    turned = packed.T
    damped = jnp.where(row >= col, packed, turned) + jnp.where(row == col, level, 0.0)
    diagonal = edge[0:1] / tokens + level_after
    following = jnp.where(row == col, diagonal, jnp.where(row < col, packed, turned))
    final = last_ref[0] == 1
    following = jnp.where(final, jnp.where(row == col, 1.0, 0.0), following)
    cross = jnp.where(final, 0.0, owned[:B] / tokens)
    solved = jnp.concatenate(inverted(cut_panels(following)), axis=0)
    coupling = jnp.dot(cross, solved, precision=lax.Precision.HIGHEST, preferred_element_type=jnp.float32)
    coupling_ref[0] = coupling
    product = lax.dot_general(
        coupling, cross, (((1,), (1,)), ((), ())), precision=lax.Precision.HIGHEST, preferred_element_type=jnp.float32
    )
    schur = damped - product
    schur = (schur + schur.T) * 0.5
    for i, panel in enumerate(inverted(cut_panels(schur))):
        inverse_ref[0, i * PANEL : (i + 1) * PANEL, :] = panel


def solved_blocks(arrived, last, tokens, width):
    vmem = pl.BlockSpec(memory_space=pltpu.VMEM)
    return pl.pallas_call(
        partial(solve_kernel, float(tokens), float(width)),
        out_shape=[jax.ShapeDtypeStruct((1, B, B), jnp.float32)] * 2,
        in_specs=[pl.BlockSpec(memory_space=pltpu.SMEM)] + [vmem] * 4,
        out_specs=[vmem] * 2,
        name="solved_blocks",
        cost_estimate=pl.CostEstimate(flops=10**7, bytes_accessed=6 * B * B * 8, transcendentals=0),
        compiler_params=pltpu.CompilerParams(vmem_limit_bytes=16 * 2**20),
    )(last, *arrived)


def local(activations, damping):
    token_rows, local_layers, model_width = activations.shape
    group_size = lax.axis_size("dp")
    section_count = lax.axis_size("section")
    section = lax.axis_index("section")
    dp = lax.axis_index("dp")
    groups = column_groups()
    by_layer = activations.reshape(token_rows // PANEL, PANEL, local_layers, model_width).transpose(0, 2, 1, 3)
    by_layer = lax.optimization_barrier(by_layer)

    def exchanged(columns):
        return lax.all_to_all(columns, EVERY, split_axis=0, concat_axis=0, axis_index_groups=groups, tiled=True)

    x0 = exchanged(sent_columns(by_layer, damping, 0))
    x2 = lax.ppermute(x0, EVERY, following_route())
    x1 = exchanged(sent_columns(by_layer, damping, 1))
    position = jnp.stack([section == 1, (dp >> 2) & 1, (dp >> 1) & 1]).astype(jnp.int32)
    sent = partial_grams(x0, x1, x2, position)
    arrived = [lax.ppermute(sent[a * 2 + b], EVERY, home_route(a, b)) for a in range(2) for b in range(2)]
    last = jnp.logical_and(section == section_count - 1, dp // (group_size // local_layers) == local_layers - 1)
    return tuple(solved_blocks(arrived, last.astype(jnp.int32)[None], token_rows * group_size, model_width))


def solution(mesh):
    placed = (P("dp", "section", None), P("section"))
    return jax.shard_map(
        local,
        mesh=mesh,
        in_specs=placed,
        out_specs=(P(("section", "dp"), None, None), P(("section", "dp"), None, None)),
        check_vma=False,
    )
```

```python
from functools import partial

import jax
import jax.numpy as jnp
from jax import lax
from jax.experimental import pallas as pl
from jax.experimental.pallas import tpu as pltpu
from jax.sharding import PartitionSpec as P

B = 128
PANEL = 8
STEP = 16
PARTS = 3
EVERY = ("section", "dp")


def dp_index(y1, y0, xl, z2, z1, z0):
    return ((((y1 * 2 + y0) * 2 + xl) * 2 + z2) * 2 + z1) * 2 + z0


def flipped(section):
    return section // 2


BITS = [tuple((d >> s) & 1 for s in (5, 4, 3, 2, 1, 0)) for d in range(64)]


def column_groups():
    groups = []
    for section in range(4):
        for z2 in range(2):
            for z1 in range(2):
                groups.append(
                    [
                        section * 64 + dp_index(m >> 3, (m >> 2) & 1, ((m >> 1) & 1) ^ flipped(section), z2, z1, m & 1)
                        for m in range(16)
                    ]
                )
    return groups


def following_route():
    route = []
    for section in range(1, 4):
        turn = flipped(section) ^ flipped(section - 1)
        for d, (y1, y0, xl, z2, z1, z0) in enumerate(BITS):
            route.append((section * 64 + d, (section - 1) * 64 + dp_index(y1, y0, xl ^ turn, z2, z1, z0)))
    return route


def home_route(a, b):
    route = []
    for section in range(4):
        turn = flipped(section)
        for d, (y1, y0, xl, z2, z1, z0) in enumerate(BITS):
            route.append((section * 64 + d, section * 64 + dp_index(z1 ^ a, y0, xl ^ turn, z2 ^ b, y1, z0)))
    return route


def member_block(m, zz):
    z1, y0, xl, z0 = m >> 3, (m >> 2) & 1, (m >> 1) & 1, m & 1
    return (((y0 * 2 + xl) * 2 + zz) * 2 + z1) * 2 + z0


def parts_of(value):
    parts = []
    for _ in range(PARTS):
        part = value.astype(jnp.bfloat16)
        parts.append(part)
        value = value - part.astype(jnp.float32)
    return parts


def columns_kernel(layer, damping_ref, x_ref, out_ref):
    groups = x_ref.shape[0]
    squares = jnp.zeros((PANEL, B), jnp.float32)
    for m in range(16):
        for zz in range(2):
            k = member_block(m, zz)
            cut = x_ref[:, layer, :, k * B : (k + 1) * B]
            out_ref[m, zz * groups : (zz + 1) * groups] = cut
            wide = cut.astype(jnp.float32)
            squares = squares + jnp.sum(wide * wide, axis=0)
    squares = jnp.broadcast_to(jnp.sum(squares, axis=0, keepdims=True), (PANEL, B))
    damping = jnp.full((PANEL, B), damping_ref[layer])
    row = lax.broadcasted_iota(jnp.int32, (PANEL, B), 0)
    extra = jnp.zeros((PANEL, B), jnp.float32)
    for i, part in enumerate(parts_of(squares) + parts_of(damping)):
        extra = jnp.where(row == i, part.astype(jnp.float32), extra)
    extra = extra.astype(jnp.bfloat16)
    for m in range(16):
        out_ref[m, 2 * groups] = extra


def sent_columns(x, damping, layer):
    groups = x.shape[0]
    vmem = pl.BlockSpec(memory_space=pltpu.VMEM)
    out = pl.pallas_call(
        partial(columns_kernel, layer),
        out_shape=jax.ShapeDtypeStruct((16, 2 * groups + 1, PANEL, B), jnp.bfloat16),
        in_specs=[pl.BlockSpec(memory_space=pltpu.SMEM), vmem],
        out_specs=vmem,
        name="sent_columns",
        cost_estimate=pl.CostEstimate(flops=2 * 2**20, bytes_accessed=2 * 2**21, transcendentals=0),
        compiler_params=pltpu.CompilerParams(vmem_limit_bytes=16 * 2**20),
    )(damping, x)
    return out.reshape(16, (2 * groups + 1) * PANEL, B)


def level_rows(x_ref):
    rows = x_ref.shape[1]
    total = jnp.zeros((PANEL, B), jnp.float32)
    for j in range(x_ref.shape[0]):
        total = total + x_ref[j, rows - PANEL :, :].astype(jnp.float32)
    last = x_ref[0, rows - PANEL :, :].astype(jnp.float32)
    squares = jnp.sum(total[:PARTS], axis=0, keepdims=True)
    damping = jnp.sum(last[PARTS : 2 * PARTS], axis=0, keepdims=True)
    return squares, damping * 0.25


def tokens_of(x_ref, zz, turn=0):
    rows = (x_ref.shape[1] - PANEL) // 2
    return jnp.concatenate([x_ref[j ^ (turn * 2), zz * rows : (zz + 1) * rows, :] for j in range(x_ref.shape[0])], axis=0)


def gram(left, right):
    return lax.dot_general(left, right, (((0,), (0,)), ((), ())), preferred_element_type=jnp.float32)


def own_kernel(x_ref, gram_ref, level_ref, kept_ref):
    squares, damping = level_rows(x_ref)
    level_ref[0:1, :] = squares
    level_ref[1:2, :] = damping
    level_ref[2:PANEL, :] = jnp.zeros((PANEL - 2, B), jnp.float32)
    for zz in range(2):
        x = tokens_of(x_ref, zz)
        kept_ref[zz] = x
        gram_ref[zz] = gram(x, x)


def own_grams(x):
    vmem = pl.BlockSpec(memory_space=pltpu.VMEM)
    return pl.pallas_call(
        own_kernel,
        out_shape=[
            jax.ShapeDtypeStruct((2, B, B), jnp.float32),
            jax.ShapeDtypeStruct((PANEL, B), jnp.float32),
            jax.ShapeDtypeStruct((2, x.shape[0] * (x.shape[1] - PANEL) // 2, B), jnp.bfloat16),
        ],
        in_specs=[vmem],
        out_specs=[vmem] * 3,
        name="own_grams",
        cost_estimate=pl.CostEstimate(flops=4 * 3072 * B * B, bytes_accessed=2 * 3072 * B * 2, transcendentals=0),
        compiler_params=pltpu.CompilerParams(vmem_limit_bytes=16 * 2**20),
    )(x)


def gram_kernel(pos_ref, d0_ref, level_ref, x0_ref, x1_ref, x2_ref, *out_refs):
    turn, z2, z1 = pos_ref[0], pos_ref[1], pos_ref[2]
    row = lax.broadcasted_iota(jnp.int32, (B, B), 0)
    col = lax.broadcasted_iota(jnp.int32, (B, B), 1)
    levels = [(level_ref[0:1, :], level_ref[1:2, :])] + [level_rows(x_ref) for x_ref in (x1_ref, x2_ref)]
    for zz in range(2):
        x0, x1, x2 = x0_ref[zz], tokens_of(x1_ref, zz), tokens_of(x2_ref, zz, turn)
        middle = gram(x1, jnp.concatenate([x1, x2], axis=1))
        d0, d1, c12 = d0_ref[zz], middle[:, :B], middle[:, B:]
        c01 = gram(x1, x0).T
        d2 = gram(x2, x2)
        for layer, (d, n, c) in enumerate(((d0, d1, c01), (d1, d2, c12))):
            packed = jnp.where(row >= col, d, n)
            edge = jnp.sum(jnp.where(row == col, n, 0.0), axis=0, keepdims=True)
            for b in range(2):
                for a in range(2):

                    @pl.when(jnp.logical_and((z2 ^ b) == zz, (z1 ^ a) == layer))
                    def _():
                        out = out_refs[a * 2 + b]
                        out[0:B, :] = c
                        out[B : 2 * B, :] = packed
                        out[2 * B : 2 * B + 1, :] = edge
                        for i in range(2):
                            out[2 * B + 1 + i : 2 * B + 2 + i, :] = levels[layer + i][0]
                            out[2 * B + 3 + i : 2 * B + 4 + i, :] = levels[layer + i][1]
                        out[2 * B + 5 : 2 * B + 8, :] = jnp.zeros((3, B), jnp.float32)


def partial_grams(d0, level0, x0, x1, x2, position):
    vmem = pl.BlockSpec(memory_space=pltpu.VMEM)
    return pl.pallas_call(
        gram_kernel,
        out_shape=[jax.ShapeDtypeStruct((2 * B + PANEL, B), jnp.float32)] * 4,
        in_specs=[pl.BlockSpec(memory_space=pltpu.SMEM)] + [vmem] * 5,
        out_specs=[vmem] * 4,
        name="partial_grams",
        cost_estimate=pl.CostEstimate(flops=8 * 3072 * B * B * 2, bytes_accessed=6 * 3072 * B * 2, transcendentals=0),
        compiler_params=pltpu.CompilerParams(vmem_limit_bytes=24 * 2**20),
    )(position, d0, level0, x0, x1, x2)


def inverted(panels):
    sub = lax.broadcasted_iota(jnp.int32, (STEP, B), 0)
    lane = lax.broadcasted_iota(jnp.int32, (STEP, B), 1)
    count = B // STEP
    panels = list(panels)
    nothing = jnp.zeros((STEP, B), jnp.float32)

    def spread(panel, first):
        return [jnp.broadcast_to(panel[:, first + j : first + j + 1], (STEP, B)) for j in range(STEP)]

    for k in range(count):
        first = k * STEP
        here = jnp.logical_and(lane >= first, lane < first + STEP)
        own = spread(panels[k], first)
        panel = jnp.where(here, jnp.where(lane - first == sub, 1.0, 0.0), panels[k])
        for j in range(STEP):
            scale = 1.0 / own[j][j : j + 1, :]
            for q in range(j + 1, STEP):
                top = own[q][j : j + 1, :] * scale
                own[q] = jnp.where(sub == j, top, own[q] - own[j] * top)
            top = panel[j : j + 1, :] * scale
            panel = jnp.where(sub == j, top, panel - own[j] * top)
        following = k + 1 if k + 1 < count else None
        rows = [i for i in range(count) if i != k and i != following]
        left = jnp.concatenate([jnp.where(here, panels[i], 0.0) for i in rows], axis=0)
        right = jnp.concatenate([panel if i == k else nothing for i in range(count)], axis=0)
        product = jnp.dot(left, right, precision=lax.Precision.HIGHEST, preferred_element_type=jnp.float32)
        for at, i in enumerate(rows):
            panels[i] = jnp.where(here, 0.0, panels[i]) - product[at * STEP : (at + 1) * STEP]
        if following is not None:
            coefs = spread(panels[following], first)
            rest = jnp.where(here, 0.0, panels[following])
            for j in range(STEP):
                rest = rest - coefs[j] * panel[j : j + 1, :]
            panels[following] = rest
        panels[k] = panel
    return panels


def cut_panels(square):
    return [square[i * STEP : (i + 1) * STEP, :] for i in range(B // STEP)]


def solve_kernel(tokens, width, last_ref, *refs):
    arrived, (inverse_ref, coupling_ref) = refs[:4], refs[4:]
    owned = arrived[0][...] + arrived[1][...] + arrived[2][...] + arrived[3][...]
    row = lax.broadcasted_iota(jnp.int32, (B, B), 0)
    col = lax.broadcasted_iota(jnp.int32, (B, B), 1)
    edge = owned[2 * B :]
    mean = jnp.sum(edge, axis=1, keepdims=True) / tokens / width
    level, level_after = mean[1:2] * edge[3:4], mean[2:3] * edge[4:5]
    packed = owned[B : 2 * B] / tokens
    turned = packed.T
    damped = jnp.where(row >= col, packed, turned) + jnp.where(row == col, level, 0.0)
    diagonal = edge[0:1] / tokens + level_after
    following = jnp.where(row == col, diagonal, jnp.where(row < col, packed, turned))
    final = last_ref[0] == 1
    following = jnp.where(final, jnp.where(row == col, 1.0, 0.0), following)
    cross = jnp.where(final, 0.0, owned[:B] / tokens)
    solved = jnp.concatenate(inverted(cut_panels(following)), axis=0)
    coupling = jnp.dot(cross, solved, precision=lax.Precision.HIGHEST, preferred_element_type=jnp.float32)
    coupling_ref[0] = coupling
    product = lax.dot_general(
        coupling, cross, (((1,), (1,)), ((), ())), precision=lax.Precision.HIGHEST, preferred_element_type=jnp.float32
    )
    schur = damped - product
    schur = (schur + schur.T) * 0.5
    for i, panel in enumerate(inverted(cut_panels(schur))):
        inverse_ref[0, i * STEP : (i + 1) * STEP, :] = panel


def solved_blocks(arrived, last, tokens, width):
    vmem = pl.BlockSpec(memory_space=pltpu.VMEM)
    return pl.pallas_call(
        partial(solve_kernel, float(tokens), float(width)),
        out_shape=[jax.ShapeDtypeStruct((1, B, B), jnp.float32)] * 2,
        in_specs=[pl.BlockSpec(memory_space=pltpu.SMEM)] + [vmem] * 4,
        out_specs=[vmem] * 2,
        name="solved_blocks",
        cost_estimate=pl.CostEstimate(flops=10**7, bytes_accessed=6 * B * B * 8, transcendentals=0),
        compiler_params=pltpu.CompilerParams(vmem_limit_bytes=16 * 2**20),
    )(last, *arrived)


def local(activations, damping):
    token_rows, local_layers, model_width = activations.shape
    group_size = lax.axis_size("dp")
    section_count = lax.axis_size("section")
    section = lax.axis_index("section")
    dp = lax.axis_index("dp")
    groups = column_groups()
    by_layer = activations.reshape(token_rows // PANEL, PANEL, local_layers, model_width).transpose(0, 2, 1, 3)
    by_layer = lax.optimization_barrier(by_layer)

    def exchanged(columns):
        return lax.all_to_all(columns, EVERY, split_axis=0, concat_axis=0, axis_index_groups=groups, tiled=True)

    x0 = exchanged(sent_columns(by_layer, damping, 0))
    x2 = lax.ppermute(x0, EVERY, following_route())
    x1 = exchanged(sent_columns(by_layer, damping, 1))
    position = jnp.stack([section == 1, (dp >> 2) & 1, (dp >> 1) & 1]).astype(jnp.int32)
    d0, level0, kept = own_grams(x0)
    sent = partial_grams(d0, level0, kept, x1, x2, position)
    arrived = [lax.ppermute(sent[a * 2 + b], EVERY, home_route(a, b)) for a in range(2) for b in range(2)]
    last = jnp.logical_and(section == section_count - 1, dp // (group_size // local_layers) == local_layers - 1)
    return tuple(solved_blocks(arrived, last.astype(jnp.int32)[None], token_rows * group_size, model_width))


def solution(mesh):
    placed = (P("dp", "section", None), P("section"))
    return jax.shard_map(
        local,
        mesh=mesh,
        in_specs=placed,
        out_specs=(P(("section", "dp"), None, None), P(("section", "dp"), None, None)),
        check_vma=False,
    )
```

```python
from functools import partial

import jax
import jax.numpy as jnp
from jax import lax
from jax.experimental import pallas as pl
from jax.experimental.pallas import tpu as pltpu
from jax.sharding import PartitionSpec as P

B = 128
PANEL = 8
STEP = 16
PARTS = 3
EVERY = ("section", "dp")


def dp_index(y1, y0, xl, z2, z1, z0):
    return ((((y1 * 2 + y0) * 2 + xl) * 2 + z2) * 2 + z1) * 2 + z0


def flipped(section):
    return section // 2


BITS = [tuple((d >> s) & 1 for s in (5, 4, 3, 2, 1, 0)) for d in range(64)]


Y_OF = {(0, 0): 1, (0, 1): 3, (1, 0): 2, (1, 1): 0}
CODE_OF = {y: code for code, y in Y_OF.items()}


def member_index(m, turn, z2, z1):
    y = Y_OF[((m >> 2) & 1, m >> 3)]
    return dp_index(y >> 1, y & 1, ((m >> 1) & 1) ^ turn, z2, z1, m & 1)


def column_groups():
    groups = []
    for section in range(4):
        for z2 in range(2):
            for z1 in range(2):
                groups.append(
                    [
                        section * 64 + member_index(m, flipped(section), z2, z1)
                        for m in range(16)
                    ]
                )
    return groups


def following_route():
    route = []
    for section in range(1, 4):
        turn = flipped(section) ^ flipped(section - 1)
        for d, (y1, y0, xl, z2, z1, z0) in enumerate(BITS):
            route.append((section * 64 + d, (section - 1) * 64 + dp_index(y1, y0, xl ^ turn, z2, z1, z0)))
    return route


def home_route(a, b):
    route = []
    for section in range(4):
        turn = flipped(section)
        for d, (y1, y0, xl, z2, z1, z0) in enumerate(BITS):
            home_y0, home_z1 = CODE_OF[y1 * 2 + y0]
            home = dp_index(z1 ^ a, home_y0, xl ^ turn, z2 ^ b, home_z1, z0)
            route.append((section * 64 + d, section * 64 + home))
    return route


def member_block(m, zz):
    z1, y0, xl, z0 = m >> 3, (m >> 2) & 1, (m >> 1) & 1, m & 1
    return (((y0 * 2 + xl) * 2 + zz) * 2 + z1) * 2 + z0


def parts_of(value):
    parts = []
    for _ in range(PARTS):
        part = value.astype(jnp.bfloat16)
        parts.append(part)
        value = value - part.astype(jnp.float32)
    return parts


def columns_kernel(layer, damping_ref, x_ref, out_ref):
    groups = x_ref.shape[0]
    squares = jnp.zeros((PANEL, B), jnp.float32)
    for m in range(16):
        for zz in range(2):
            k = member_block(m, zz)
            cut = x_ref[:, layer, :, k * B : (k + 1) * B]
            out_ref[m, zz * groups : (zz + 1) * groups] = cut
            wide = cut.astype(jnp.float32)
            squares = squares + jnp.sum(wide * wide, axis=0)
    squares = jnp.broadcast_to(jnp.sum(squares, axis=0, keepdims=True), (PANEL, B))
    damping = jnp.full((PANEL, B), damping_ref[layer])
    row = lax.broadcasted_iota(jnp.int32, (PANEL, B), 0)
    extra = jnp.zeros((PANEL, B), jnp.float32)
    for i, part in enumerate(parts_of(squares) + parts_of(damping)):
        extra = jnp.where(row == i, part.astype(jnp.float32), extra)
    extra = extra.astype(jnp.bfloat16)
    for m in range(16):
        out_ref[m, 2 * groups] = extra


def sent_columns(x, damping, layer):
    groups = x.shape[0]
    vmem = pl.BlockSpec(memory_space=pltpu.VMEM)
    out = pl.pallas_call(
        partial(columns_kernel, layer),
        out_shape=jax.ShapeDtypeStruct((16, 2 * groups + 1, PANEL, B), jnp.bfloat16),
        in_specs=[pl.BlockSpec(memory_space=pltpu.SMEM), vmem],
        out_specs=vmem,
        name="sent_columns",
        cost_estimate=pl.CostEstimate(flops=2 * 2**20, bytes_accessed=2 * 2**21, transcendentals=0),
        compiler_params=pltpu.CompilerParams(vmem_limit_bytes=16 * 2**20),
    )(damping, x)
    return out.reshape(16, (2 * groups + 1) * PANEL, B)


def level_rows(x_ref):
    rows = x_ref.shape[1]
    total = jnp.zeros((PANEL, B), jnp.float32)
    for j in range(x_ref.shape[0]):
        total = total + x_ref[j, rows - PANEL :, :].astype(jnp.float32)
    last = x_ref[0, rows - PANEL :, :].astype(jnp.float32)
    squares = jnp.sum(total[:PARTS], axis=0, keepdims=True)
    damping = jnp.sum(last[PARTS : 2 * PARTS], axis=0, keepdims=True)
    return squares, damping * 0.25


def tokens_of(x_ref, zz, turn=0):
    rows = (x_ref.shape[1] - PANEL) // 2
    return jnp.concatenate([x_ref[j ^ (turn * 2), zz * rows : (zz + 1) * rows, :] for j in range(x_ref.shape[0])], axis=0)


def gram(left, right):
    return lax.dot_general(left, right, (((0,), (0,)), ((), ())), preferred_element_type=jnp.float32)


def own_kernel(x_ref, gram_ref, level_ref):
    squares, damping = level_rows(x_ref)
    level_ref[0:1, :] = squares
    level_ref[1:2, :] = damping
    level_ref[2:PANEL, :] = jnp.zeros((PANEL - 2, B), jnp.float32)
    for zz in range(2):
        x = tokens_of(x_ref, zz)
        gram_ref[zz] = gram(x, x)


def own_grams(x):
    vmem = pl.BlockSpec(memory_space=pltpu.VMEM)
    return pl.pallas_call(
        own_kernel,
        out_shape=[
            jax.ShapeDtypeStruct((2, B, B), jnp.float32),
            jax.ShapeDtypeStruct((PANEL, B), jnp.float32),
        ],
        in_specs=[vmem],
        out_specs=[vmem] * 2,
        name="own_grams",
        cost_estimate=pl.CostEstimate(flops=4 * 3072 * B * B, bytes_accessed=2 * 3072 * B * 2, transcendentals=0),
        compiler_params=pltpu.CompilerParams(vmem_limit_bytes=8 * 2**20),
    )(x)


def gram_kernel(pos_ref, d0_ref, level_ref, x0_ref, x1_ref, x2_ref, *refs):
    out_refs, (held_ref, sem) = refs[:4], refs[4:]
    turn, z2, z1 = pos_ref[0], pos_ref[1], pos_ref[2]
    copy = pltpu.make_async_copy(x0_ref, held_ref, sem)
    copy.start()
    row = lax.broadcasted_iota(jnp.int32, (B, B), 0)
    col = lax.broadcasted_iota(jnp.int32, (B, B), 1)
    afters = []
    for zz in range(2):
        x1, x2 = tokens_of(x1_ref, zz), tokens_of(x2_ref, zz, turn)
        afters.append(gram(x2, jnp.concatenate([x1, x2], axis=1)))
    levels = [(level_ref[0:1, :], level_ref[1:2, :]), level_rows(x1_ref), level_rows(x2_ref)]
    copy.wait()
    for zz in range(2):
        x0, x1 = tokens_of(held_ref, zz), tokens_of(x1_ref, zz)
        first, after = gram(x1, jnp.concatenate([x0, x1], axis=1)), afters[zz]
        c01, d1, c12, d2, d0 = first[:, :B], first[:, B:], after[:, :B], after[:, B:], d0_ref[zz]
        for layer, (d, n, c) in enumerate(((d0, d1, c01), (d1, d2, c12))):
            packed = jnp.where(row >= col, d, n)
            edge = jnp.sum(jnp.where(row == col, n, 0.0), axis=0, keepdims=True)
            for b in range(2):
                for a in range(2):

                    @pl.when(jnp.logical_and((z2 ^ b) == zz, (z1 ^ a) == layer))
                    def _():
                        out = out_refs[a * 2 + b]
                        out[0:B, :] = c
                        out[B : 2 * B, :] = packed
                        out[2 * B : 2 * B + 1, :] = edge
                        for i in range(2):
                            out[2 * B + 1 + i : 2 * B + 2 + i, :] = levels[layer + i][0]
                            out[2 * B + 3 + i : 2 * B + 4 + i, :] = levels[layer + i][1]
                        out[2 * B + 5 : 2 * B + 8, :] = jnp.zeros((3, B), jnp.float32)


def partial_grams(d0, level0, x0, x1, x2, position):
    vmem = pl.BlockSpec(memory_space=pltpu.VMEM)
    return pl.pallas_call(
        gram_kernel,
        out_shape=[jax.ShapeDtypeStruct((2 * B + PANEL, B), jnp.float32)] * 4,
        in_specs=[pl.BlockSpec(memory_space=pltpu.SMEM)]
        + [vmem] * 2
        + [pl.BlockSpec(memory_space=pltpu.MemorySpace.HBM)]
        + [vmem] * 2,
        out_specs=[vmem] * 4,
        scratch_shapes=[pltpu.VMEM(x0.shape, jnp.bfloat16), pltpu.SemaphoreType.DMA(())],
        name="partial_grams",
        cost_estimate=pl.CostEstimate(flops=8 * 3072 * B * B * 2, bytes_accessed=6 * 3072 * B * 2, transcendentals=0),
        compiler_params=pltpu.CompilerParams(vmem_limit_bytes=16 * 2**20),
    )(position, d0, level0, x0, x1, x2)


def inverted(panels):
    sub = lax.broadcasted_iota(jnp.int32, (STEP, B), 0)
    lane = lax.broadcasted_iota(jnp.int32, (STEP, B), 1)
    count = B // STEP
    panels = list(panels)
    nothing = jnp.zeros((STEP, B), jnp.float32)

    def spread(panel, first):
        return [jnp.broadcast_to(panel[:, first + j : first + j + 1], (STEP, B)) for j in range(STEP)]

    for k in range(count):
        first = k * STEP
        here = jnp.logical_and(lane >= first, lane < first + STEP)
        own = spread(panels[k], first)
        panel = jnp.where(here, jnp.where(lane - first == sub, 1.0, 0.0), panels[k])
        for j in range(STEP):
            scale = 1.0 / own[j][j : j + 1, :]
            for q in range(j + 1, STEP):
                top = own[q][j : j + 1, :] * scale
                own[q] = jnp.where(sub == j, top, own[q] - own[j] * top)
            top = panel[j : j + 1, :] * scale
            panel = jnp.where(sub == j, top, panel - own[j] * top)
        following = k + 1 if k + 1 < count else None
        rows = [i for i in range(count) if i != k and i != following]
        left = jnp.concatenate([jnp.where(here, panels[i], 0.0) for i in rows], axis=0)
        right = jnp.concatenate([panel if i == k else nothing for i in range(count)], axis=0)
        product = jnp.dot(left, right, precision=lax.Precision.HIGHEST, preferred_element_type=jnp.float32)
        for at, i in enumerate(rows):
            panels[i] = jnp.where(here, 0.0, panels[i]) - product[at * STEP : (at + 1) * STEP]
        if following is not None:
            coefs = spread(panels[following], first)
            rest = jnp.where(here, 0.0, panels[following])
            for j in range(STEP):
                rest = rest - coefs[j] * panel[j : j + 1, :]
            panels[following] = rest
        panels[k] = panel
    return panels


def cut_panels(square):
    return [square[i * STEP : (i + 1) * STEP, :] for i in range(B // STEP)]


def solve_kernel(tokens, width, last_ref, *refs):
    arrived, (inverse_ref, coupling_ref) = refs[:4], refs[4:]
    owned = arrived[0][...] + arrived[1][...] + arrived[2][...] + arrived[3][...]
    row = lax.broadcasted_iota(jnp.int32, (B, B), 0)
    col = lax.broadcasted_iota(jnp.int32, (B, B), 1)
    edge = owned[2 * B :]
    mean = jnp.sum(edge, axis=1, keepdims=True) / tokens / width
    level, level_after = mean[1:2] * edge[3:4], mean[2:3] * edge[4:5]
    packed = owned[B : 2 * B] / tokens
    turned = packed.T
    damped = jnp.where(row >= col, packed, turned) + jnp.where(row == col, level, 0.0)
    diagonal = edge[0:1] / tokens + level_after
    following = jnp.where(row == col, diagonal, jnp.where(row < col, packed, turned))
    final = last_ref[0] == 1
    following = jnp.where(final, jnp.where(row == col, 1.0, 0.0), following)
    cross = jnp.where(final, 0.0, owned[:B].T / tokens)
    solved = jnp.concatenate(inverted(cut_panels(following)), axis=0)
    coupling = jnp.dot(cross, solved, precision=lax.Precision.HIGHEST, preferred_element_type=jnp.float32)
    coupling_ref[0] = coupling
    product = lax.dot_general(
        coupling, cross, (((1,), (1,)), ((), ())), precision=lax.Precision.HIGHEST, preferred_element_type=jnp.float32
    )
    schur = damped - product
    schur = (schur + schur.T) * 0.5
    for i, panel in enumerate(inverted(cut_panels(schur))):
        inverse_ref[0, i * STEP : (i + 1) * STEP, :] = panel


def solved_blocks(arrived, last, tokens, width):
    vmem = pl.BlockSpec(memory_space=pltpu.VMEM)
    return pl.pallas_call(
        partial(solve_kernel, float(tokens), float(width)),
        out_shape=[jax.ShapeDtypeStruct((1, B, B), jnp.float32)] * 2,
        in_specs=[pl.BlockSpec(memory_space=pltpu.SMEM)] + [vmem] * 4,
        out_specs=[vmem] * 2,
        name="solved_blocks",
        cost_estimate=pl.CostEstimate(flops=10**7, bytes_accessed=6 * B * B * 8, transcendentals=0),
        compiler_params=pltpu.CompilerParams(vmem_limit_bytes=16 * 2**20),
    )(last, *arrived)


def local(activations, damping):
    token_rows, local_layers, model_width = activations.shape
    group_size = lax.axis_size("dp")
    section_count = lax.axis_size("section")
    section = lax.axis_index("section")
    dp = lax.axis_index("dp")
    groups = column_groups()
    by_layer = activations.reshape(token_rows // PANEL, PANEL, local_layers, model_width).transpose(0, 2, 1, 3)
    by_layer = lax.optimization_barrier(by_layer)

    def exchanged(columns):
        return lax.all_to_all(columns, EVERY, split_axis=0, concat_axis=0, axis_index_groups=groups, tiled=True)

    x0 = exchanged(sent_columns(by_layer, damping, 0))
    x2 = lax.ppermute(x0, EVERY, following_route())
    x1 = exchanged(sent_columns(by_layer, damping, 1))
    position = jnp.stack([section == 1, (dp >> 2) & 1, (dp >> 1) & 1]).astype(jnp.int32)
    d0, level0 = own_grams(x0)
    sent = partial_grams(d0, level0, x0, x1, x2, position)
    arrived = [lax.ppermute(sent[a * 2 + b], EVERY, home_route(a, b)) for a in range(2) for b in range(2)]
    last = jnp.logical_and(section == section_count - 1, dp // (group_size // local_layers) == local_layers - 1)
    return tuple(solved_blocks(arrived, last.astype(jnp.int32)[None], token_rows * group_size, model_width))


def solution(mesh):
    placed = (P("dp", "section", None), P("section"))
    return jax.shard_map(
        local,
        mesh=mesh,
        in_specs=placed,
        out_specs=(P(("section", "dp"), None, None), P(("section", "dp"), None, None)),
        check_vma=False,
    )
```

```python
from functools import partial

import jax
import jax.numpy as jnp
from jax import lax
from jax.experimental import pallas as pl
from jax.experimental.pallas import tpu as pltpu
from jax.sharding import PartitionSpec as P

B = 128
PANEL = 8
STEP = 16
PARTS = 3
EVERY = ("section", "dp")


def dp_index(y1, y0, xl, z2, z1, z0):
    return ((((y1 * 2 + y0) * 2 + xl) * 2 + z2) * 2 + z1) * 2 + z0


def flipped(section):
    return section // 2


BITS = [tuple((d >> s) & 1 for s in (5, 4, 3, 2, 1, 0)) for d in range(64)]


Y_OF = {(0, 0): 1, (0, 1): 3, (1, 0): 2, (1, 1): 0}
CODE_OF = {y: code for code, y in Y_OF.items()}


def member_index(m, turn, z2, z1):
    y = Y_OF[((m >> 2) & 1, m >> 3)]
    return dp_index(y >> 1, y & 1, ((m >> 1) & 1) ^ turn, z2, z1, m & 1)


def column_groups():
    groups = []
    for section in range(4):
        for z2 in range(2):
            for z1 in range(2):
                groups.append(
                    [
                        section * 64 + member_index(m, flipped(section), z2, z1)
                        for m in range(16)
                    ]
                )
    return groups


def following_route():
    route = []
    for section in range(1, 4):
        turn = flipped(section) ^ flipped(section - 1)
        for d, (y1, y0, xl, z2, z1, z0) in enumerate(BITS):
            route.append((section * 64 + d, (section - 1) * 64 + dp_index(y1, y0, xl ^ turn, z2, z1, z0)))
    return route


def home_route(a, b):
    route = []
    for section in range(4):
        turn = flipped(section)
        for d, (y1, y0, xl, z2, z1, z0) in enumerate(BITS):
            home_y0, home_z1 = CODE_OF[y1 * 2 + y0]
            home = dp_index(z1 ^ a, home_y0, xl ^ turn, z2 ^ b, home_z1, z0)
            route.append((section * 64 + d, section * 64 + home))
    return route


def member_block(m, zz):
    z1, y0, xl, z0 = m >> 3, (m >> 2) & 1, (m >> 1) & 1, m & 1
    return (((y0 * 2 + xl) * 2 + zz) * 2 + z1) * 2 + z0


def parts_of(value):
    parts = []
    for _ in range(PARTS):
        part = value.astype(jnp.bfloat16)
        parts.append(part)
        value = value - part.astype(jnp.float32)
    return parts


def columns_kernel(layer, damping_ref, x_ref, out_ref):
    groups = x_ref.shape[0]
    squares = jnp.zeros((PANEL, B), jnp.float32)
    for m in range(16):
        for zz in range(2):
            k = member_block(m, zz)
            cut = x_ref[:, layer, :, k * B : (k + 1) * B]
            out_ref[m, zz * groups : (zz + 1) * groups] = cut
            wide = cut.astype(jnp.float32)
            squares = squares + jnp.sum(wide * wide, axis=0)
    squares = jnp.broadcast_to(jnp.sum(squares, axis=0, keepdims=True), (PANEL, B))
    damping = jnp.full((PANEL, B), damping_ref[layer])
    row = lax.broadcasted_iota(jnp.int32, (PANEL, B), 0)
    extra = jnp.zeros((PANEL, B), jnp.float32)
    for i, part in enumerate(parts_of(squares) + parts_of(damping)):
        extra = jnp.where(row == i, part.astype(jnp.float32), extra)
    extra = extra.astype(jnp.bfloat16)
    for m in range(16):
        out_ref[m, 2 * groups] = extra


def sent_columns(x, damping, layer):
    groups = x.shape[0]
    vmem = pl.BlockSpec(memory_space=pltpu.VMEM)
    out = pl.pallas_call(
        partial(columns_kernel, layer),
        out_shape=jax.ShapeDtypeStruct((16, 2 * groups + 1, PANEL, B), jnp.bfloat16),
        in_specs=[pl.BlockSpec(memory_space=pltpu.SMEM), vmem],
        out_specs=vmem,
        name="sent_columns",
        cost_estimate=pl.CostEstimate(flops=2 * 2**20, bytes_accessed=2 * 2**21, transcendentals=0),
        compiler_params=pltpu.CompilerParams(vmem_limit_bytes=16 * 2**20),
    )(damping, x)
    return out.reshape(16, (2 * groups + 1) * PANEL, B)


def level_rows(x_ref):
    rows = x_ref.shape[1]
    total = jnp.zeros((PANEL, B), jnp.float32)
    for j in range(x_ref.shape[0]):
        total = total + x_ref[j, rows - PANEL :, :].astype(jnp.float32)
    last = x_ref[0, rows - PANEL :, :].astype(jnp.float32)
    squares = jnp.sum(total[:PARTS], axis=0, keepdims=True)
    damping = jnp.sum(last[PARTS : 2 * PARTS], axis=0, keepdims=True)
    return squares, damping * 0.25


def tokens_of(x_ref, zz, turn=0):
    rows = (x_ref.shape[1] - PANEL) // 2
    return jnp.concatenate([x_ref[j ^ (turn * 2), zz * rows : (zz + 1) * rows, :] for j in range(x_ref.shape[0])], axis=0)


def gram(left, right):
    return lax.dot_general(left, right, (((0,), (0,)), ((), ())), preferred_element_type=jnp.float32)


def own_kernel(x_ref, gram_ref, level_ref):
    squares, damping = level_rows(x_ref)
    level_ref[0:1, :] = squares
    level_ref[1:2, :] = damping
    level_ref[2:PANEL, :] = jnp.zeros((PANEL - 2, B), jnp.float32)
    for zz in range(2):
        x = tokens_of(x_ref, zz)
        gram_ref[zz] = gram(x, x)


def own_grams(x):
    vmem = pl.BlockSpec(memory_space=pltpu.VMEM)
    return pl.pallas_call(
        own_kernel,
        out_shape=[
            jax.ShapeDtypeStruct((2, B, B), jnp.float32),
            jax.ShapeDtypeStruct((PANEL, B), jnp.float32),
        ],
        in_specs=[vmem],
        out_specs=[vmem] * 2,
        name="own_grams",
        cost_estimate=pl.CostEstimate(flops=4 * 3072 * B * B, bytes_accessed=2 * 3072 * B * 2, transcendentals=0),
        compiler_params=pltpu.CompilerParams(vmem_limit_bytes=8 * 2**20),
    )(x)


def gram_kernel(pos_ref, d0_ref, level_ref, x0_ref, x1_ref, x2_ref, *refs):
    out_refs, (held_ref, sem) = refs[:4], refs[4:]
    turn, z2, z1 = pos_ref[0], pos_ref[1], pos_ref[2]
    copy = pltpu.make_async_copy(x0_ref, held_ref, sem)
    copy.start()
    row = lax.broadcasted_iota(jnp.int32, (B, B), 0)
    col = lax.broadcasted_iota(jnp.int32, (B, B), 1)
    afters = []
    for zz in range(2):
        x1, x2 = tokens_of(x1_ref, zz), tokens_of(x2_ref, zz, turn)
        afters.append(gram(x2, jnp.concatenate([x1, x2], axis=1)))
    levels = [(level_ref[0:1, :], level_ref[1:2, :]), level_rows(x1_ref), level_rows(x2_ref)]
    copy.wait()
    for zz in range(2):
        x0, x1 = tokens_of(held_ref, zz), tokens_of(x1_ref, zz)
        first, after = gram(x1, jnp.concatenate([x0, x1], axis=1)), afters[zz]
        c01, d1, c12, d2, d0 = first[:, :B], first[:, B:], after[:, :B], after[:, B:], d0_ref[zz]
        for layer, (d, n, c) in enumerate(((d0, d1, c01), (d1, d2, c12))):
            packed = jnp.where(row >= col, d, n)
            edge = jnp.sum(jnp.where(row == col, n, 0.0), axis=0, keepdims=True)
            for b in range(2):
                for a in range(2):

                    @pl.when(jnp.logical_and((z2 ^ b) == zz, (z1 ^ a) == layer))
                    def _():
                        out = out_refs[a * 2 + b]
                        out[0:B, :] = c
                        out[B : 2 * B, :] = packed
                        out[2 * B : 2 * B + 1, :] = edge
                        for i in range(2):
                            out[2 * B + 1 + i : 2 * B + 2 + i, :] = levels[layer + i][0]
                            out[2 * B + 3 + i : 2 * B + 4 + i, :] = levels[layer + i][1]
                        out[2 * B + 5 : 2 * B + 8, :] = jnp.zeros((3, B), jnp.float32)


def partial_grams(d0, level0, x0, x1, x2, position):
    vmem = pl.BlockSpec(memory_space=pltpu.VMEM)
    return pl.pallas_call(
        gram_kernel,
        out_shape=[jax.ShapeDtypeStruct((2 * B + PANEL, B), jnp.float32)] * 4,
        in_specs=[pl.BlockSpec(memory_space=pltpu.SMEM)]
        + [vmem] * 2
        + [pl.BlockSpec(memory_space=pltpu.MemorySpace.HBM)]
        + [vmem] * 2,
        out_specs=[vmem] * 4,
        scratch_shapes=[pltpu.VMEM(x0.shape, jnp.bfloat16), pltpu.SemaphoreType.DMA(())],
        name="partial_grams",
        cost_estimate=pl.CostEstimate(flops=8 * 3072 * B * B * 2, bytes_accessed=6 * 3072 * B * 2, transcendentals=0),
        compiler_params=pltpu.CompilerParams(vmem_limit_bytes=16 * 2**20),
    )(position, d0, level0, x0, x1, x2)


def inverted(panels):
    sub = lax.broadcasted_iota(jnp.int32, (STEP, B), 0)
    lane = lax.broadcasted_iota(jnp.int32, (STEP, B), 1)
    count = B // STEP
    panels = list(panels)
    nothing = jnp.zeros((STEP, B), jnp.float32)

    def spread(panel, first):
        return [jnp.broadcast_to(panel[:, first + j : first + j + 1], (STEP, B)) for j in range(STEP)]

    for k in range(count):
        first = k * STEP
        here = jnp.logical_and(lane >= first, lane < first + STEP)
        own = spread(panels[k], first)
        panel = jnp.where(here, jnp.where(lane - first == sub, 1.0, 0.0), panels[k])
        for j in range(STEP):
            scale = 1.0 / own[j][j : j + 1, :]
            for q in range(j + 1, STEP):
                top = own[q][j : j + 1, :] * scale
                own[q] = jnp.where(sub == j, top, own[q] - own[j] * top)
            top = panel[j : j + 1, :] * scale
            panel = jnp.where(sub == j, top, panel - own[j] * top)
        close = [i for i in range(k + 1, min(k + 1 + 1, count))]
        rows = [i for i in range(count) if i != k and i not in close]
        coefs = [spread(panels[i], first) for i in close]
        for i, weights in zip(close, coefs):
            rest = jnp.where(here, 0.0, panels[i])
            for j in range(STEP):
                rest = rest - weights[j] * panel[j : j + 1, :]
            panels[i] = rest
        if rows:
            left = jnp.concatenate([jnp.where(here, panels[i], 0.0) for i in rows], axis=0)
            right = jnp.concatenate([panel if i == k else nothing for i in range(count)], axis=0)
            product = jnp.dot(left, right, precision=lax.Precision.HIGHEST, preferred_element_type=jnp.float32)
            for at, i in enumerate(rows):
                panels[i] = jnp.where(here, 0.0, panels[i]) - product[at * STEP : (at + 1) * STEP]
        panels[k] = panel
    return panels


def cut_panels(square):
    return [square[i * STEP : (i + 1) * STEP, :] for i in range(B // STEP)]


def solve_kernel(tokens, width, last_ref, *refs):
    arrived, (inverse_ref, coupling_ref) = refs[:4], refs[4:]
    owned = arrived[0][...] + arrived[1][...] + arrived[2][...] + arrived[3][...]
    row = lax.broadcasted_iota(jnp.int32, (B, B), 0)
    col = lax.broadcasted_iota(jnp.int32, (B, B), 1)
    edge = owned[2 * B :]
    mean = jnp.sum(edge, axis=1, keepdims=True) / tokens / width
    level, level_after = mean[1:2] * edge[3:4], mean[2:3] * edge[4:5]
    packed = owned[B : 2 * B] / tokens
    turned = packed.T
    damped = jnp.where(row >= col, packed, turned) + jnp.where(row == col, level, 0.0)
    diagonal = edge[0:1] / tokens + level_after
    following = jnp.where(row == col, diagonal, jnp.where(row < col, packed, turned))
    final = last_ref[0] == 1
    following = jnp.where(final, jnp.where(row == col, 1.0, 0.0), following)
    cross = jnp.where(final, 0.0, owned[:B].T / tokens)
    solved = jnp.concatenate(inverted(cut_panels(following)), axis=0)
    coupling = jnp.dot(cross, solved, precision=lax.Precision.HIGHEST, preferred_element_type=jnp.float32)
    coupling_ref[0] = coupling
    product = lax.dot_general(
        coupling, cross, (((1,), (1,)), ((), ())), precision=lax.Precision.HIGHEST, preferred_element_type=jnp.float32
    )
    schur = damped - product
    for i, panel in enumerate(inverted(cut_panels(schur))):
        inverse_ref[0, i * STEP : (i + 1) * STEP, :] = panel


def solved_blocks(arrived, last, tokens, width):
    vmem = pl.BlockSpec(memory_space=pltpu.VMEM)
    return pl.pallas_call(
        partial(solve_kernel, float(tokens), float(width)),
        out_shape=[jax.ShapeDtypeStruct((1, B, B), jnp.float32)] * 2,
        in_specs=[pl.BlockSpec(memory_space=pltpu.SMEM)] + [vmem] * 4,
        out_specs=[vmem] * 2,
        name="solved_blocks",
        cost_estimate=pl.CostEstimate(flops=10**7, bytes_accessed=6 * B * B * 8, transcendentals=0),
        compiler_params=pltpu.CompilerParams(vmem_limit_bytes=16 * 2**20),
    )(last, *arrived)


def local(activations, damping):
    token_rows, local_layers, model_width = activations.shape
    group_size = lax.axis_size("dp")
    section_count = lax.axis_size("section")
    section = lax.axis_index("section")
    dp = lax.axis_index("dp")
    groups = column_groups()
    by_layer = activations.reshape(token_rows // PANEL, PANEL, local_layers, model_width).transpose(0, 2, 1, 3)
    by_layer = lax.optimization_barrier(by_layer)

    def exchanged(columns):
        return lax.all_to_all(columns, EVERY, split_axis=0, concat_axis=0, axis_index_groups=groups, tiled=True)

    x0 = exchanged(sent_columns(by_layer, damping, 0))
    x2 = lax.ppermute(x0, EVERY, following_route())
    x1 = exchanged(sent_columns(by_layer, damping, 1))
    position = jnp.stack([section == 1, (dp >> 2) & 1, (dp >> 1) & 1]).astype(jnp.int32)
    d0, level0 = own_grams(x0)
    sent = partial_grams(d0, level0, x0, x1, x2, position)
    arrived = [lax.ppermute(sent[a * 2 + b], EVERY, home_route(a, b)) for a in range(2) for b in range(2)]
    last = jnp.logical_and(section == section_count - 1, dp // (group_size // local_layers) == local_layers - 1)
    return tuple(solved_blocks(arrived, last.astype(jnp.int32)[None], token_rows * group_size, model_width))


def solution(mesh):
    placed = (P("dp", "section", None), P("section"))
    return jax.shard_map(
        local,
        mesh=mesh,
        in_specs=placed,
        out_specs=(P(("section", "dp"), None, None), P(("section", "dp"), None, None)),
        check_vma=False,
    )
```
